32 devices in a mesh: dom: 8 (over y, x, core), col: 4 (over z).
Axes of the slice: x: 2, y: 2, z: 4, core: 2. Of those that a mesh axis runs over, the one named last changes fastest.
Arguments:
- features: bfloat16 [65536, 1024], P('dom', 'col')
- weight: bfloat16 [1024, 1024], P(None, 'col'), may hold values from -0.1875 to 0.1875
- out_bias: bfloat16 [1024], P('col'), may hold values from -3 to 3
- local_index: int32 [8, 64, 4], P('dom'), may hold values from 0 to 63
- local_count: int32 [8, 64], P('dom'), may hold values from 1 to 4, as said below
- local_vals: bfloat16 [8, 64, 4, 128, 128], P('dom'), may hold values from -0.1875 to 0.1875
- halo_index: int32 [8, 64, 4], P('dom'), may hold values from 0 to 31
- halo_count: int32 [8, 64], P('dom'), may hold values from 0 to 4, as said below
- halo_vals: bfloat16 [8, 64, 4, 128, 128], P('dom'), may hold values from -0.1875 to 0.1875
- send_rows: int32 [8, 8, 512], P('dom'), may hold values from 0 to 8191
- send_count: int32 [8, 8], P('dom'), may hold values from 0 to 512, as said below
Outputs:
- normalized: bfloat16 [65536, 1024], P('dom', 'col')
- channel_stats: float32 [2, 1024], P(None, 'col')
The draws below stay inside these ranges and needn't reach their ends.
Inputs may be any that keep to these rules, and one draw needn't show every extreme that they name: `local_index`: slots k >= local_count of a row tile are not used. `local_count`: every partition has a row tile with all 4 slots used. `halo_index`: slots k >= halo_count of a row tile are not used. `halo_count`: every partition has a row tile with all 4 slots used. `send_rows`: slots s >= send_count[q, p] are not used. send_count[p, p] is 0; every partition fills all 512 slots to some other partition.
All inputs are finite; a program needn't handle non-finite values.
Results may differ from the reference program's by a relative error of at most 0.0075.
Values may be sent and summed in bfloat16 or wider, within the bound.
A program may use at most 192 MiB of HBM per device.

```python
import jax
import jax.numpy as jnp
from jax import lax

F = 1024
ROWS_DEV = 8192
TILE = 128
LOCAL_SLOTS = 4
HALO_SLOTS = 4
HALO_PEER = 512
NODES = 65536
LOCAL_TILES = 64
HALO_TILES = 32
N_DOM = 8


def draw_features(key, part):
    key_base = jax.random.fold_in(key, 0)
    rising = 1.0 + 2.0 * jnp.arange(NODES, dtype=jnp.float32) / NODES
    values = jax.random.normal(key_base, (NODES, F), jnp.float32) * rising[:, None]
    return values.astype(jnp.bfloat16)


def slot_counts(key, highest, lowest):
    key_base, key_heavy, key_place = jax.random.split(key, 3)
    counts = jax.random.randint(key_base, (N_DOM, LOCAL_TILES), lowest, highest + 1)
    heavier = jax.random.randint(key_heavy, (N_DOM, 1), 0, highest)
    counts = jnp.minimum(counts + heavier, highest)
    placed = jax.random.randint(key_place, (N_DOM, 1), 0, LOCAL_TILES)
    tile_ids = jnp.arange(LOCAL_TILES)[None, :]
    return jnp.where(tile_ids == placed, highest, counts).astype(jnp.int32)


def draw_local_count(key, part):
    return slot_counts(jax.random.fold_in(key, 11), LOCAL_SLOTS, 1)


def draw_halo_count(key, part):
    return slot_counts(jax.random.fold_in(key, 23), HALO_SLOTS, 0)


def draw_send_count(key, part):
    key_base, key_target = jax.random.split(jax.random.fold_in(key, 37))
    counts = jax.random.randint(key_base, (N_DOM, N_DOM), HALO_PEER // 4, HALO_PEER + 1)
    offset = jax.random.randint(key_target, (N_DOM, 1), 1, N_DOM)
    sources = jnp.arange(N_DOM)[:, None]
    targets = jnp.arange(N_DOM)[None, :]
    counts = jnp.where(targets == (sources + offset) % N_DOM, HALO_PEER, counts)
    return jnp.where(targets == sources, 0, counts).astype(jnp.int32)


def touch_ends(entries, key, low, high):
    longest = entries.shape.index(max(entries.shape))
    spots = []
    for shift in (0, 1):
        where = [jax.random.randint(jax.random.fold_in(key, axis), (), 0, length) for axis, length in enumerate(entries.shape)]
        where[longest] = (where[longest] + shift) % entries.shape[longest]
        spots.append(tuple(where))
    return entries.at[spots[0]].set(low).at[spots[1]].set(high)


def block_levels(stream_key, shape, cuts, least, high):
    level = 1.0
    for dim, shards_of in cuts:
        draws = jax.random.uniform(jax.random.fold_in(jax.random.fold_in(stream_key, 6), dim), (shards_of,), jnp.float32, least / len(cuts), high / len(cuts))
        level = level * jnp.repeat(jnp.exp(draws), shape[dim] // shards_of).reshape((-1,) + (1,) * (len(shape) - 1 - dim))
    return level


def bell_draw(stream_key, dims, deviation, reach, cuts=(), kind=jnp.bfloat16):
    entries = deviation * jax.random.normal(stream_key, dims, jnp.float32)
    if cuts:
        entries = entries * block_levels(stream_key, dims, cuts, -0.22, 0.18)
    return jnp.clip(entries, -reach, reach).astype(kind)


def setup_inputs(seed: int = 0) -> dict:
    arg_keys = jax.random.split(jax.random.key(seed), 12)
    features = draw_features(jax.random.fold_in(arg_keys[11], 71), 0)
    weight = bell_draw(arg_keys[1], (F, F), F ** -0.5, 0.1875, ((1, 4),))
    out_bias = bell_draw(arg_keys[2], (F,), 0.5, 3.0, ((0, 4),))
    local_index = touch_ends(jax.random.randint(arg_keys[3], (N_DOM, LOCAL_TILES, LOCAL_SLOTS), 0, LOCAL_TILES), jax.random.fold_in(arg_keys[3], 1), 0, LOCAL_TILES - 1).astype(jnp.int32)
    local_count = draw_local_count(jax.random.fold_in(arg_keys[11], 71), 0)
    local_vals = bell_draw(arg_keys[5], (N_DOM, LOCAL_TILES, LOCAL_SLOTS, TILE, TILE), (TILE * (LOCAL_SLOTS + HALO_SLOTS)) ** -0.5, 0.1875, ((0, 8),))
    halo_index = touch_ends(jax.random.randint(arg_keys[6], (N_DOM, LOCAL_TILES, HALO_SLOTS), 0, HALO_TILES), jax.random.fold_in(arg_keys[6], 1), 0, HALO_TILES - 1).astype(jnp.int32)
    halo_count = draw_halo_count(jax.random.fold_in(arg_keys[11], 71), 0)
    halo_vals = bell_draw(arg_keys[8], (N_DOM, LOCAL_TILES, HALO_SLOTS, TILE, TILE), (TILE * (LOCAL_SLOTS + HALO_SLOTS)) ** -0.5, 0.1875, ((0, 8),))
    send_rows = touch_ends(jax.random.randint(arg_keys[9], (N_DOM, N_DOM, HALO_PEER), 0, ROWS_DEV), jax.random.fold_in(arg_keys[9], 1), 0, ROWS_DEV - 1).astype(jnp.int32)
    send_count = draw_send_count(jax.random.fold_in(arg_keys[11], 71), 0)
    return {"features": features, "weight": weight, "out_bias": out_bias, "local_index": local_index, "local_count": local_count, "local_vals": local_vals, "halo_index": halo_index, "halo_count": halo_count, "halo_vals": halo_vals, "send_rows": send_rows, "send_count": send_count}


epsilon = 1e-06

def tile_product(sources, tile_index, tile_count, tile_vals, slot_total):
    gathered = sources[tile_index]
    keep_mask = jnp.arange(slot_total)[None, :] < tile_count[:, None]
    masked = jnp.where(keep_mask[:, :, None, None], tile_vals, jnp.zeros_like(tile_vals))
    return jnp.einsum('tkij,tkjc->tic', masked.astype(jnp.float32), gathered.astype(jnp.float32))

def reference(features, weight, out_bias, local_index, local_count, local_vals, halo_index, halo_count, halo_vals, send_rows, send_count):
    blocks = features.reshape(N_DOM, ROWS_DEV, F)
    slot_ids = jnp.arange(HALO_PEER)
    sources_ids = jnp.arange(N_DOM)

    def aggregate(partition):
        chosen = blocks[sources_ids[:, None], send_rows[:, partition, :]]
        keep_mask = slot_ids[None, :] < send_count[:, partition][:, None]
        halo_tiles = jnp.where(keep_mask[:, :, None], chosen, jnp.zeros_like(chosen)).reshape(HALO_TILES, TILE, F)
        own_tiles = blocks[partition].reshape(LOCAL_TILES, TILE, F)
        summed = tile_product(own_tiles, local_index[partition], local_count[partition], local_vals[partition], LOCAL_SLOTS)
        summed = summed + tile_product(halo_tiles, halo_index[partition], halo_count[partition], halo_vals[partition], HALO_SLOTS)
        return summed.reshape(ROWS_DEV, F).astype(jnp.bfloat16)
    spread = lax.map(aggregate, jnp.arange(N_DOM)).reshape(NODES, F)
    mixed_rows = jnp.dot(spread, weight, preferred_element_type=jnp.float32) + out_bias.astype(jnp.float32)
    active = jnp.maximum(mixed_rows, 0.0)
    row_power = lax.optimization_barrier(jnp.mean(active * active, axis=1, keepdims=True))
    scaled = active * lax.rsqrt(row_power + epsilon)
    channel_mean = lax.optimization_barrier(jnp.sum(scaled, axis=0)) / NODES
    channel_var = lax.optimization_barrier(jnp.sum(scaled * scaled, axis=0)) / NODES - channel_mean * channel_mean
    return (scaled.astype(jnp.bfloat16), jnp.stack([channel_mean, channel_var]))
```

```python
import functools

import jax
import jax.numpy as jnp
from jax import lax
from jax.experimental import pallas as pl
from jax.experimental.pallas import tpu as pltpu
from jax.sharding import PartitionSpec as P

TILE = 128
MESH = pl.DeviceIdType.MESH
CHUNK_TILES = 2
epsilon = 1e-06


def remote(src, dst, send_sem, recv_sem, device):
    return pltpu.make_async_remote_copy(
        src_ref=src,
        dst_ref=dst,
        send_sem=send_sem,
        recv_sem=recv_sem,
        device_id=device,
        device_id_type=MESH,
    )


def kernel(
    n_dom,
    n_col,
    node_total,
    feat_hbm,
    weight_ref,
    bias_ref,
    lidx,
    lcnt,
    lvals_hbm,
    hidx,
    hcnt,
    hvals_hbm,
    srows,
    scnt,
    out_hbm,
    stat_ref,
    xb,
    xf,
    stage,
    outgoing,
    halo,
    lvals,
    hvals,
    wfull,
    bfull,
    tx,
    rx,
    tx2,
    acc,
    part,
    part_in,
    colpart,
    colpart_in,
    in_sem,
    halo_s,
    halo_r,
    w_s,
    w_r,
    wp_s,
    wp_r,
    b_s,
    b_r,
    p1_s,
    p1_r,
    p2_s,
    p2_r,
    own_sem,
    sd_s,
    sd_r,
    sc_s,
    sc_r,
):
    d = lax.axis_index("dom")
    z = lax.axis_index("col")
    rows, width = xf.shape
    slot_total = srows.shape[1]
    k_local = lvals.shape[1]
    k_halo = hvals.shape[1]
    f_total = weight_ref.shape[0]
    tiles_q = rows // TILE // n_col
    rows_q = tiles_q * TILE
    ct = CHUNK_TILES
    r_chunk = ct * TILE
    steps = tiles_q // ct
    per_peer = slot_total // TILE
    half = f_total // 2

    feat_copy = pltpu.make_async_copy(feat_hbm, xb, in_sem.at[0])
    feat_copy.start()

    barrier = pltpu.get_barrier_semaphore()
    for o in range(1, n_dom):
        pl.semaphore_signal(barrier, inc=1, device_id=(lax.rem(d + o, n_dom), z), device_id_type=MESH)
    for o in range(1, n_col):
        pl.semaphore_signal(barrier, inc=1, device_id=(d, lax.rem(z + o, n_col)), device_id_type=MESH)
    pl.semaphore_wait(barrier, n_dom - 1 + n_col - 1)

    core = lax.rem(d, 2)
    mate = d + 1 - 2 * core
    my_half = pl.ds(pl.multiple_of(core * half, half), half)

    def w_copy(o):
        return remote(
            weight_ref.at[my_half],
            wfull.at[z, my_half],
            w_s.at[o - 1],
            w_r.at[o - 1],
            (d, lax.rem(z + o, n_col)),
        )

    def w_pass(o):
        src = lax.rem(z + n_col - o, n_col)
        return remote(
            wfull.at[src, my_half], wfull.at[src, my_half], wp_s.at[o - 1], wp_r.at[o - 1], (mate, z)
        )

    def b_copy(o):
        return remote(
            bias_ref, bfull.at[z], b_s.at[o - 1], b_r.at[o - 1], (d, lax.rem(z + o, n_col))
        )

    for o in range(1, n_col):
        w_copy(o).start()
        b_copy(o).start()

    feat_copy.wait()
    lv_copy = pltpu.make_async_copy(lvals_hbm, lvals, in_sem.at[1])
    hv_copy = pltpu.make_async_copy(hvals_hbm, hvals, in_sem.at[2])
    lv_copy.start()
    hv_copy.start()

    @pl.loop(0, rows // TILE)
    def _(i):
        at = pl.ds(pl.multiple_of(i * TILE, TILE), TILE)
        xf[at, :] = xb[i].astype(jnp.float32)

    def halo_copy(o):
        return remote(
            outgoing.at[o],
            halo.at[pl.ds(d * per_peer, per_peer)],
            halo_s.at[o],
            halo_r.at[o],
            (lax.rem(d + o, n_dom), z),
        )

    @pl.loop(1, n_dom)
    def _(o):
        peer = lax.rem(d + o, n_dom)

        @pl.loop(0, slot_total // 16)
        def _(g):
            for k in range(16):
                at = g * 16 + k
                stage[at] = xf[srows[peer, at]]

        used = lax.broadcasted_iota(jnp.int32, (slot_total, width), 0) < scnt[0, peer]
        sent = jnp.where(used, stage[...], 0.0).astype(outgoing.dtype)
        outgoing[o] = sent.reshape(slot_total // TILE, TILE, width)
        halo_copy(o).start()

    halo[pl.ds(d * per_peer, per_peer)] = jnp.zeros((per_peer, TILE, width), halo.dtype)
    wfull[z] = weight_ref[...]
    bfull[z] = bias_ref[...]

    for o in range(1, n_col):
        w_copy(o).wait_recv()
        w_pass(o).start()

    lv_copy.wait()
    hv_copy.wait()

    @pl.loop(1, n_dom)
    def _(o):
        halo_copy(o).wait()

    def kept(count, k):
        one = jnp.minimum(jnp.maximum(count - k, 0), 1).astype(jnp.float32)
        return jnp.broadcast_to(one, (TILE, TILE)).astype(jnp.bfloat16)

    def tile_rows(t):
        lhs, rhs = [], []
        n_loc, n_hal = lcnt[0, t], hcnt[0, t]
        for k in range(k_local):
            v = lvals[t, k]
            lhs.append(v * kept(n_loc, k))
            rhs.append(xb[lidx[t, k]])
        for k in range(k_halo):
            v = hvals[t, k]
            lhs.append(v * kept(n_hal, k))
            rhs.append(halo[hidx[t, k]])
        total = jnp.dot(
            jnp.concatenate(lhs, axis=1),
            jnp.concatenate(rhs, axis=0),
            preferred_element_type=jnp.float32,
        )
        return total.astype(jnp.bfloat16)

    my_cols = pl.ds(pl.multiple_of(z * width, width), width)

    def p1_copy(s, o):
        return remote(
            tx.at[s, o - 1],
            rx.at[s, :, my_cols],
            p1_s.at[s, o - 1],
            p1_r.at[s, o - 1],
            (d, lax.rem(z + o, n_col)),
        )

    @pl.loop(0, steps)
    def _(s):
        for o in range(1, n_col):
            q = lax.rem(z + o, n_col)
            for c in range(ct):
                tx[s, o - 1, c * TILE : (c + 1) * TILE, :] = tile_rows(q * tiles_q + s * ct + c)
            p1_copy(s, o).start()
        for c in range(ct):
            rx[s, c * TILE : (c + 1) * TILE, my_cols] = tile_rows(z * tiles_q + s * ct + c)

    for o in range(1, n_col):
        w_pass(o).wait()
        b_copy(o).wait()
        w_copy(o).wait_send()

    acc[...] = jnp.zeros_like(acc)

    def out_rows(s):
        return pl.ds(pl.multiple_of(z * rows_q + s * r_chunk, r_chunk), r_chunk)

    def p2_copy(s, o):
        q = lax.rem(z + o, n_col)
        return remote(
            tx2.at[s, q],
            out_hbm.at[out_rows(s)],
            p2_s.at[s, o - 1],
            p2_r.at[s, o - 1],
            (d, q),
        )

    def own_copy(s):
        return pltpu.make_async_copy(tx2.at[s, z], out_hbm.at[out_rows(s)], own_sem.at[s])

    @pl.loop(0, steps)
    def _(s):
        for o in range(1, n_col):
            p1_copy(s, o).wait_recv()
        power = jnp.zeros((r_chunk, 1), jnp.float32)
        active = []
        for j in range(n_col):
            y = jnp.dot(rx[s], wfull[j], preferred_element_type=jnp.float32)
            y = jnp.maximum(y + bfull[j][0:1, :].astype(jnp.float32), 0.0)
            power = power + jnp.sum(y * y, axis=1, keepdims=True)
            active.append(y)
        factor = lax.rsqrt(power / f_total + epsilon)
        for j in range(n_col):
            scaled = active[j] * factor
            tx2[s, j] = scaled.astype(jnp.bfloat16)
            grouped = scaled.reshape(r_chunk // 8, 8, width)
            acc[j, 0] += jnp.sum(grouped, axis=0)
            acc[j, 1] += jnp.sum(grouped * grouped, axis=0)
        for o in range(1, n_col):
            p2_copy(s, o).start()
        own_copy(s).start()

    for j in range(n_col):
        part[j] = jnp.concatenate(
            [
                jnp.sum(acc[j, 0], axis=0, keepdims=True),
                jnp.sum(acc[j, 1], axis=0, keepdims=True),
                jnp.zeros((6, width), jnp.float32),
            ],
            axis=0,
        )

    def sd_copy(o):
        return remote(part, part_in.at[o], sd_s.at[o], sd_r.at[o], (lax.rem(d + o, n_dom), z))

    @pl.loop(1, n_dom)
    def _(o):
        sd_copy(o).start()

    part_in[0] = part[...]

    @pl.loop(1, n_dom)
    def _(o):
        sd_copy(o).wait()

    colpart[...] = jnp.sum(part_in[...], axis=0)

    def sc_copy(o):
        q = lax.rem(z + o, n_col)
        return remote(colpart.at[q], colpart_in.at[o], sc_s.at[o - 1], sc_r.at[o - 1], (d, q))

    for o in range(1, n_col):
        sc_copy(o).start()
    colpart_in[0] = colpart[z]

    @pl.loop(0, steps)
    def _(s):
        for o in range(1, n_col):
            p1_copy(s, o).wait_send()
            p2_copy(s, o).wait()
        own_copy(s).wait()

    for o in range(1, n_col):
        sc_copy(o).wait()
    totals = jnp.sum(colpart_in[...], axis=0) / node_total
    mean = totals[0:1, :]
    stat_ref[...] = jnp.concatenate([mean, totals[1:2, :] - mean * mean], axis=0)


def on_device(
    features,
    weight,
    out_bias,
    local_index,
    local_count,
    local_vals,
    halo_index,
    halo_count,
    halo_vals,
    send_rows,
    send_count,
):
    rows, width = features.shape
    n_dom = lax.axis_size("dom")
    n_col = lax.axis_size("col")
    slot_total = send_rows.shape[2]
    f_total = weight.shape[0]
    steps = rows // TILE // n_col // CHUNK_TILES
    r_chunk = CHUNK_TILES * TILE
    bias_rows = jnp.broadcast_to(out_bias[None, :], (16, width))
    any_spec = pl.BlockSpec(memory_space=pl.ANY)
    vmem = pl.BlockSpec(memory_space=pltpu.VMEM)
    smem = pl.BlockSpec(memory_space=pltpu.SMEM)
    bf16, f32 = jnp.bfloat16, jnp.float32
    dma = pltpu.SemaphoreType.DMA
    normalized, stats = pl.pallas_call(
        functools.partial(kernel, n_dom, n_col, rows * n_dom),
        out_shape=(
            jax.ShapeDtypeStruct((rows, width), bf16),
            jax.ShapeDtypeStruct((2, width), f32),
        ),
        in_specs=[any_spec, vmem, vmem, smem, smem, any_spec, smem, smem, any_spec, smem, smem],
        out_specs=(any_spec, vmem),
        scratch_shapes=[
            pltpu.VMEM((rows // TILE, TILE, width), bf16),
            pltpu.VMEM((rows, width), f32),
            pltpu.VMEM((slot_total, width), f32),
            pltpu.VMEM((n_dom, slot_total // TILE, TILE, width), bf16),
            pltpu.VMEM((n_dom * slot_total // TILE, TILE, width), bf16),
            pltpu.VMEM(local_vals.shape[1:], bf16),
            pltpu.VMEM(halo_vals.shape[1:], bf16),
            pltpu.VMEM((n_col, f_total, width), bf16),
            pltpu.VMEM((n_col, 16, width), bf16),
            pltpu.VMEM((steps, n_col - 1, r_chunk, width), bf16),
            pltpu.VMEM((steps, r_chunk, n_col * width), bf16),
            pltpu.VMEM((steps, n_col, r_chunk, width), bf16),
            pltpu.VMEM((n_col, 2, 8, width), f32),
            pltpu.VMEM((n_col, 8, width), f32),
            pltpu.VMEM((n_dom, n_col, 8, width), f32),
            pltpu.VMEM((n_col, 8, width), f32),
            pltpu.VMEM((n_col, 8, width), f32),
            dma((3,)),
            dma((n_dom,)),
            dma((n_dom,)),
            dma((n_col - 1,)),
            dma((n_col - 1,)),
            dma((n_col - 1,)),
            dma((n_col - 1,)),
            dma((n_col - 1,)),
            dma((n_col - 1,)),
            dma((steps, n_col - 1)),
            dma((steps, n_col - 1)),
            dma((steps, n_col - 1)),
            dma((steps, n_col - 1)),
            dma((steps,)),
            dma((n_dom,)),
            dma((n_dom,)),
            dma((n_col - 1,)),
            dma((n_col - 1,)),
        ],
        compiler_params=pltpu.CompilerParams(
            collective_id=0, has_side_effects=True, vmem_limit_bytes=67043328
        ),
    )(
        features.reshape(rows // TILE, TILE, width),
        weight,
        bias_rows,
        local_index[0],
        local_count,
        local_vals[0],
        halo_index[0],
        halo_count,
        halo_vals[0],
        send_rows[0],
        send_count,
    )
    return normalized, stats


def solution(mesh):
    in_specs = (
        P("dom", "col"),
        P(None, "col"),
        P("col"),
        P("dom", None, None),
        P("dom", None),
        P("dom", None, None, None, None),
        P("dom", None, None),
        P("dom", None),
        P("dom", None, None, None, None),
        P("dom", None, None),
        P("dom", None),
    )
    out_specs = (P("dom", "col"), P(None, "col"))
    return jax.shard_map(
        on_device, mesh=mesh, in_specs=in_specs, out_specs=out_specs, check_vma=False
    )
```

```python
import functools

import jax
import jax.numpy as jnp
from jax import lax
from jax.experimental import pallas as pl
from jax.experimental.pallas import tpu as pltpu
from jax.sharding import PartitionSpec as P

TILE = 128
MESH = pl.DeviceIdType.MESH
CHUNK_TILES = 2
epsilon = 1e-06


def remote(src, dst, send_sem, recv_sem, device):
    return pltpu.make_async_remote_copy(
        src_ref=src,
        dst_ref=dst,
        send_sem=send_sem,
        recv_sem=recv_sem,
        device_id=device,
        device_id_type=MESH,
    )


def kernel(
    n_dom,
    n_col,
    node_total,
    feat_hbm,
    weight_ref,
    bias_ref,
    lidx,
    lcnt,
    lvals_hbm,
    hidx,
    hcnt,
    hvals_hbm,
    srows,
    scnt,
    out_hbm,
    stat_ref,
    xb,
    xf,
    stage,
    outgoing,
    halo,
    lvals,
    hvals,
    wfull,
    bfull,
    tx,
    rx,
    tx2,
    acc,
    part,
    part_in,
    colpart,
    colpart_in,
    in_sem,
    halo_s,
    halo_r,
    w_s,
    w_r,
    wp_s,
    wp_r,
    b_s,
    b_r,
    p1_s,
    p1_r,
    p2_s,
    p2_r,
    own_sem,
    sd_s,
    sd_r,
    sc_s,
    sc_r,
):
    d = lax.axis_index("dom")
    z = lax.axis_index("col")
    rows, width = xf.shape
    slot_total = srows.shape[1]
    k_local = lvals.shape[1]
    k_halo = hvals.shape[1]
    f_total = weight_ref.shape[0]
    tiles_q = rows // TILE // n_col
    rows_q = tiles_q * TILE
    ct = CHUNK_TILES
    r_chunk = ct * TILE
    steps = tiles_q // ct
    per_peer = slot_total // TILE
    half = f_total // 2

    pieces = in_sem.shape[0] - 2
    piece = rows // TILE // pieces

    def feat_copy(i):
        at = pl.ds(i * piece, piece)
        return pltpu.make_async_copy(feat_hbm.at[at], xb.at[at], in_sem.at[2 + i])

    for i in range(pieces):
        feat_copy(i).start()
    bfull[z] = jnp.broadcast_to(bias_ref[...], bfull.shape[1:])

    barrier = pltpu.get_barrier_semaphore()
    for o in range(1, n_dom):
        pl.semaphore_signal(barrier, inc=1, device_id=(lax.rem(d + o, n_dom), z), device_id_type=MESH)
    for o in range(1, n_col):
        pl.semaphore_signal(barrier, inc=1, device_id=(d, lax.rem(z + o, n_col)), device_id_type=MESH)
    pl.semaphore_wait(barrier, n_dom - 1 + n_col - 1)

    core = lax.rem(d, 2)
    mate = d + 1 - 2 * core
    my_half = pl.ds(pl.multiple_of(core * half, half), half)

    def w_copy(o):
        return remote(
            weight_ref.at[my_half],
            wfull.at[z, my_half],
            w_s.at[o - 1],
            w_r.at[o - 1],
            (d, lax.rem(z + o, n_col)),
        )

    def w_pass(o):
        src = lax.rem(z + n_col - o, n_col)
        return remote(
            wfull.at[src, my_half], wfull.at[src, my_half], wp_s.at[o - 1], wp_r.at[o - 1], (mate, z)
        )

    def b_copy(o):
        return remote(
            bfull.at[z], bfull.at[z], b_s.at[o - 1], b_r.at[o - 1], (d, lax.rem(z + o, n_col))
        )

    for o in range(1, n_col):
        w_copy(o).start()

    lv_copy = pltpu.make_async_copy(lvals_hbm, lvals, in_sem.at[0])
    hv_copy = pltpu.make_async_copy(hvals_hbm, hvals, in_sem.at[1])
    lv_copy.start()
    hv_copy.start()

    @pl.loop(0, pieces)
    def _(i):
        feat_copy(i).wait()
        for j in range(piece):
            t = i * piece + j
            at = pl.ds(pl.multiple_of(t * TILE, TILE), TILE)
            xf[at, :] = xb[t].astype(jnp.float32)

    def peer_of(o):
        return lax.rem(d + (1 - 2 * core) * o + n_dom, n_dom)

    def halo_copy(o):
        return remote(
            outgoing.at[o],
            halo.at[pl.ds(d * per_peer, per_peer)],
            halo_s.at[o],
            halo_r.at[o],
            (peer_of(o), z),
        )

    @pl.loop(0, n_dom - 1)
    def _(i):
        o = lax.rem(i + 1, n_dom - 1) + 1
        peer = peer_of(o)

        @pl.loop(0, slot_total // 16)
        def _(g):
            for k in range(16):
                at = g * 16 + k
                stage[at] = xf[srows[peer, at]]

        used = lax.broadcasted_iota(jnp.int32, (slot_total, width), 0) < scnt[0, peer]
        sent = jnp.where(used, stage[...], 0.0).astype(outgoing.dtype)
        outgoing[o] = sent.reshape(slot_total // TILE, TILE, width)
        halo_copy(o).start()

    halo[pl.ds(d * per_peer, per_peer)] = jnp.zeros((per_peer, TILE, width), halo.dtype)
    wfull[z] = weight_ref[...]

    for o in range(1, n_col):
        w_copy(o).wait_recv()
        w_pass(o).start()
        b_copy(o).start()

    lv_copy.wait()
    hv_copy.wait()

    @pl.loop(1, n_dom)
    def _(o):
        halo_copy(o).wait()

    def kept(count, k):
        one = jnp.minimum(jnp.maximum(count - k, 0), 1).astype(jnp.float32)
        return jnp.broadcast_to(one, (TILE, TILE)).astype(jnp.bfloat16)

    def tile_rows(t):
        lhs, rhs = [], []
        n_loc, n_hal = lcnt[0, t], hcnt[0, t]
        for k in range(k_local):
            v = lvals[t, k]
            lhs.append(v * kept(n_loc, k))
            rhs.append(xb[lidx[k, t]])
        for k in range(k_halo):
            v = hvals[t, k]
            lhs.append(v * kept(n_hal, k))
            rhs.append(halo[hidx[k, t]])
        total = jnp.dot(
            jnp.concatenate(lhs, axis=1),
            jnp.concatenate(rhs, axis=0),
            preferred_element_type=jnp.float32,
        )
        return total.astype(jnp.bfloat16)

    my_cols = pl.ds(pl.multiple_of(z * width, width), width)

    def p1_copy(s, o):
        return remote(
            tx.at[s, o - 1],
            rx.at[s, :, my_cols],
            p1_s.at[s, o - 1],
            p1_r.at[s, o - 1],
            (d, lax.rem(z + o, n_col)),
        )

    @pl.loop(0, steps)
    def _(s):
        for o in range(1, n_col):
            q = lax.rem(z + o, n_col)
            for c in range(ct):
                tx[s, o - 1, c * TILE : (c + 1) * TILE, :] = tile_rows(q * tiles_q + s * ct + c)
            p1_copy(s, o).start()
        for c in range(ct):
            rx[s, c * TILE : (c + 1) * TILE, my_cols] = tile_rows(z * tiles_q + s * ct + c)

    for o in range(1, n_col):
        w_pass(o).wait()
        b_copy(o).wait()
        w_copy(o).wait_send()

    acc[...] = jnp.zeros_like(acc)

    def out_rows(s):
        return pl.ds(pl.multiple_of(z * rows_q + s * r_chunk, r_chunk), r_chunk)

    def p2_copy(s, o):
        q = lax.rem(z + o, n_col)
        return remote(
            tx2.at[s, q],
            out_hbm.at[out_rows(s)],
            p2_s.at[s, o - 1],
            p2_r.at[s, o - 1],
            (d, q),
        )

    def own_copy(s):
        return pltpu.make_async_copy(tx2.at[s, z], out_hbm.at[out_rows(s)], own_sem.at[s])

    @pl.loop(0, steps)
    def _(s):
        for o in range(1, n_col):
            p1_copy(s, o).wait_recv()
        power = jnp.zeros((r_chunk, 1), jnp.float32)
        active = []
        for j in range(n_col):
            y = jnp.dot(rx[s], wfull[j], preferred_element_type=jnp.float32)
            y = jnp.maximum(y + bfull[j][0:1, :].astype(jnp.float32), 0.0)
            power = power + jnp.sum(y * y, axis=1, keepdims=True)
            active.append(y)
        factor = lax.rsqrt(power / f_total + epsilon)
        for j in range(n_col):
            scaled = active[j] * factor
            tx2[s, j] = scaled.astype(jnp.bfloat16)
            grouped = scaled.reshape(r_chunk // 8, 8, width)
            acc[j, 0] += jnp.sum(grouped, axis=0)
            acc[j, 1] += jnp.sum(grouped * grouped, axis=0)
        for o in range(1, n_col):
            p2_copy(s, o).start()
        own_copy(s).start()

    for j in range(n_col):
        part[j] = jnp.concatenate(
            [
                jnp.sum(acc[j, 0], axis=0, keepdims=True),
                jnp.sum(acc[j, 1], axis=0, keepdims=True),
                jnp.zeros((6, width), jnp.float32),
            ],
            axis=0,
        )

    def sd_copy(o):
        return remote(part, part_in.at[o], sd_s.at[o], sd_r.at[o], (lax.rem(d + o, n_dom), z))

    @pl.loop(1, n_dom)
    def _(o):
        sd_copy(o).start()

    part_in[0] = part[...]

    @pl.loop(1, n_dom)
    def _(o):
        sd_copy(o).wait()

    colpart[...] = jnp.sum(part_in[...], axis=0)

    def sc_copy(o):
        q = lax.rem(z + o, n_col)
        return remote(colpart.at[q], colpart_in.at[o], sc_s.at[o - 1], sc_r.at[o - 1], (d, q))

    for o in range(1, n_col):
        sc_copy(o).start()
    colpart_in[0] = colpart[z]

    @pl.loop(0, steps)
    def _(s):
        for o in range(1, n_col):
            p1_copy(s, o).wait_send()
            p2_copy(s, o).wait()
        own_copy(s).wait()

    for o in range(1, n_col):
        sc_copy(o).wait()
    totals = jnp.sum(colpart_in[...], axis=0) / node_total
    mean = totals[0:1, :]
    stat_ref[...] = jnp.concatenate([mean, totals[1:2, :] - mean * mean], axis=0)


def on_device(
    features,
    weight,
    out_bias,
    local_index,
    local_count,
    local_vals,
    halo_index,
    halo_count,
    halo_vals,
    send_rows,
    send_count,
):
    rows, width = features.shape
    n_dom = lax.axis_size("dom")
    n_col = lax.axis_size("col")
    slot_total = send_rows.shape[2]
    f_total = weight.shape[0]
    steps = rows // TILE // n_col // CHUNK_TILES
    r_chunk = CHUNK_TILES * TILE
    any_spec = pl.BlockSpec(memory_space=pl.ANY)
    vmem = pl.BlockSpec(memory_space=pltpu.VMEM)
    smem = pl.BlockSpec(memory_space=pltpu.SMEM)
    bf16, f32 = jnp.bfloat16, jnp.float32
    dma = pltpu.SemaphoreType.DMA
    normalized, stats = pl.pallas_call(
        functools.partial(kernel, n_dom, n_col, rows * n_dom),
        out_shape=(
            jax.ShapeDtypeStruct((rows, width), bf16),
            jax.ShapeDtypeStruct((2, width), f32),
        ),
        in_specs=[any_spec, vmem, vmem, smem, smem, any_spec, smem, smem, any_spec, smem, smem],
        out_specs=(any_spec, vmem),
        scratch_shapes=[
            pltpu.VMEM((rows // TILE, TILE, width), bf16),
            pltpu.VMEM((rows, width), f32),
            pltpu.VMEM((slot_total, width), f32),
            pltpu.VMEM((n_dom, slot_total // TILE, TILE, width), bf16),
            pltpu.VMEM((n_dom * slot_total // TILE, TILE, width), bf16),
            pltpu.VMEM(local_vals.shape[1:], bf16),
            pltpu.VMEM(halo_vals.shape[1:], bf16),
            pltpu.VMEM((n_col, f_total, width), bf16),
            pltpu.VMEM((n_col, 16, width), bf16),
            pltpu.VMEM((steps, n_col - 1, r_chunk, width), bf16),
            pltpu.VMEM((steps, r_chunk, n_col * width), bf16),
            pltpu.VMEM((steps, n_col, r_chunk, width), bf16),
            pltpu.VMEM((n_col, 2, 8, width), f32),
            pltpu.VMEM((n_col, 8, width), f32),
            pltpu.VMEM((n_dom, n_col, 8, width), f32),
            pltpu.VMEM((n_col, 8, width), f32),
            pltpu.VMEM((n_col, 8, width), f32),
            dma((10 if rows // TILE % 8 == 0 else 3,)),
            dma((n_dom,)),
            dma((n_dom,)),
            dma((n_col - 1,)),
            dma((n_col - 1,)),
            dma((n_col - 1,)),
            dma((n_col - 1,)),
            dma((n_col - 1,)),
            dma((n_col - 1,)),
            dma((steps, n_col - 1)),
            dma((steps, n_col - 1)),
            dma((steps, n_col - 1)),
            dma((steps, n_col - 1)),
            dma((steps,)),
            dma((n_dom,)),
            dma((n_dom,)),
            dma((n_col - 1,)),
            dma((n_col - 1,)),
        ],
        compiler_params=pltpu.CompilerParams(
            collective_id=0, has_side_effects=True, vmem_limit_bytes=67043328
        ),
    )(
        features.reshape(rows // TILE, TILE, width),
        weight,
        out_bias.reshape(1, width),
        local_index[0].T,
        local_count,
        local_vals[0],
        halo_index[0].T,
        halo_count,
        halo_vals[0],
        send_rows[0],
        send_count,
    )
    return normalized, stats


def solution(mesh):
    in_specs = (
        P("dom", "col"),
        P(None, "col"),
        P("col"),
        P("dom", None, None),
        P("dom", None),
        P("dom", None, None, None, None),
        P("dom", None, None),
        P("dom", None),
        P("dom", None, None, None, None),
        P("dom", None, None),
        P("dom", None),
    )
    out_specs = (P("dom", "col"), P(None, "col"))
    return jax.shard_map(
        on_device, mesh=mesh, in_specs=in_specs, out_specs=out_specs, check_vma=False
    )
```
